32 devices in a mesh: fsdp: 4 (over x, core), ctx: 4 (over z), tp: 2 (over y).
Axes of the slice: x: 2, y: 2, z: 4, core: 2. Of those that a mesh axis runs over, the one named last changes fastest.
Arguments:
- tokens: bfloat16 [8192, 2048], P(('fsdp', 'ctx')), may hold values from -6 to 6
- cotangent: bfloat16 [8192, 2048], P(('fsdp', 'ctx')), may hold values from -6 to 6
- sequence_begin: int32 [8192], P('fsdp'), may hold values from 0 to 2047, as said below
- piece: int32 [8192], P('fsdp'), may hold values from 0 to 8, as said below
- padding_length: int32 [4], P('fsdp'), may hold values from 0 to 256, as said below
- attn_gain: bfloat16 [2048], P(('fsdp', 'ctx')), may hold values from 0.5 to 1.5
- q_gain: bfloat16 [128], P(('fsdp', 'ctx')), may hold values from 0.5 to 2
- k_gain: bfloat16 [128], P(('fsdp', 'ctx')), may hold values from 0.5 to 2
- w_query: bfloat16 [2048, 2048], P(('fsdp', 'ctx'), 'tp'), may hold values from -0.125 to 0.125
- key_weight: bfloat16 [2048, 1024], P(('fsdp', 'ctx'), 'tp'), may hold values from -0.125 to 0.125
- value_weight: bfloat16 [2048, 1024], P(('fsdp', 'ctx'), 'tp'), may hold values from -0.125 to 0.125
- w_out: bfloat16 [2048, 2048], P(('fsdp', 'ctx'), 'tp'), may hold values from -1 to 1
- mlp_gain: bfloat16 [2048], P(('fsdp', 'ctx')), may hold values from 0.5 to 1.5
- w_gate: bfloat16 [2048, 6144], P(('fsdp', 'ctx'), 'tp'), may hold values from -0.125 to 0.125
- w_up: bfloat16 [2048, 6144], P(('fsdp', 'ctx'), 'tp'), may hold values from -0.125 to 0.125
- w_down: bfloat16 [2048, 6144], P(('fsdp', 'ctx'), 'tp'), may hold values from -0.078125 to 0.078125
Outputs:
- layer_out: bfloat16 [8192, 2048], P(('fsdp', 'ctx'))
- grad_tokens: bfloat16 [8192, 2048], P(('fsdp', 'ctx'))
- grad_attn_gain: float32 [2048], P(('fsdp', 'ctx'))
- grad_q_gain: float32 [128], P(('fsdp', 'ctx'))
- grad_k_gain: float32 [128], P(('fsdp', 'ctx'))
- grad_query: float32 [2048, 2048], P(('fsdp', 'ctx'), 'tp')
- grad_key: float32 [2048, 1024], P(('fsdp', 'ctx'), 'tp')
- grad_value: float32 [2048, 1024], P(('fsdp', 'ctx'), 'tp')
- grad_out: float32 [2048, 2048], P(('fsdp', 'ctx'), 'tp')
- grad_mlp_gain: float32 [2048], P(('fsdp', 'ctx'))
- grad_gate: float32 [2048, 6144], P(('fsdp', 'ctx'), 'tp')
- grad_up: float32 [2048, 6144], P(('fsdp', 'ctx'), 'tp')
- grad_down: float32 [2048, 6144], P(('fsdp', 'ctx'), 'tp')
The draws below stay inside these ranges and needn't reach their ends.
Inputs may be any that keep to these rules, and one draw needn't show every extreme that they name: `sequence_begin`: each group of 2048 tokens holds a first sequence of 1024 or more tokens from index 0, perhaps a second one after it, then its padding tokens, which form a sequence of their own; entries are indices within the group. The 256 tokens of one aligned block of 256 positions inside one sequence may form a picture piece and then share a positive number unique in the group; all other tokens are 0. `padding_length`: some group has exactly 256 padding tokens.
All inputs are finite; a program needn't handle non-finite values.
Results may differ from the reference program's by a relative error of at most 0.02.
Values may be sent and summed in bfloat16 or wider, within the bound.
A program may use at most 256 MiB of HBM per device.

```python
import jax
import jax.numpy as jnp
from jax import lax

MODEL_WIDTH = 2048
QUERY_HEADS = 16
VALUE_HEADS = 8
HEAD_SIZE = 128
FF = 6144
PIECE = 256
GROUP_TOKENS = 2048
TOKEN_COUNT = 8192
PAD_MOST = 256
LEAST = 1024
N_FSDP = 4


def layout(key):
    subkeys = jax.random.split(key, 4)
    pad_count = jax.random.randint(subkeys[0], (N_FSDP,), 0, PAD_MOST + 1)
    chosen = jax.random.randint(subkeys[1], (), 0, N_FSDP)
    group_ids = jnp.arange(N_FSDP)
    pad_count = jnp.where(group_ids == chosen, PAD_MOST, pad_count)
    content = GROUP_TOKENS - pad_count
    split_at = jax.random.randint(subkeys[2], (N_FSDP,), LEAST, content + 1)
    position = jnp.arange(GROUP_TOKENS, dtype=jnp.int32)[None, :]
    seq_begin = jnp.where(position < split_at[:, None], 0, jnp.where(position < content[:, None], split_at[:, None], content[:, None]))
    block_id = position // PIECE
    block_lo = block_id * PIECE
    block_hi = block_lo + PIECE
    inside = (block_hi <= split_at[:, None]) | (block_lo >= split_at[:, None]) & (block_hi <= content[:, None])
    block_count = GROUP_TOKENS // PIECE
    coin_flip = jax.random.randint(subkeys[3], (N_FSDP, block_count), 0, 2)
    first_block = jnp.arange(block_count)[None, :] == 0
    coin_flip = jnp.where(first_block & (group_ids[:, None] == chosen), 1, coin_flip)
    coin_tokens = jnp.repeat(coin_flip, PIECE, axis=1)
    pieces = jnp.where(inside & (coin_tokens == 1), block_count - block_id, 0)
    return (seq_begin.reshape(-1).astype(jnp.int32), pieces.reshape(-1).astype(jnp.int32), pad_count.astype(jnp.int32))


def draw_sequence_begin(key, part):
    return layout(jax.random.fold_in(key, 17))[0]


def draw_piece(key, part):
    return layout(jax.random.fold_in(key, 17))[1]


def draw_padding_length(key, part):
    return layout(jax.random.fold_in(key, 17))[2]


def spiked(entries, key, source, target, parts, factor):
    owner, partner = [(jnp.arange(entries.shape[dim]) // (entries.shape[dim] // parts)).reshape([-1 if axis == dim else 1 for axis in range(entries.ndim)]) for dim in (source, target)]
    chosen = jax.random.permutation(key, parts)[partner]
    strong = (owner == chosen) | (owner == (partner + parts // 2) % parts)
    return jnp.where(strong, factor * entries, entries)


def block_levels(stream_key, extent, cuts, least, high):
    level = 1.0
    for dim, blocks in cuts:
        heights = jax.random.uniform(jax.random.fold_in(jax.random.fold_in(stream_key, 6), dim), (blocks,), jnp.float32, least / len(cuts), high / len(cuts))
        level = level * jnp.repeat(jnp.exp(heights), extent[dim] // blocks).reshape((-1,) + (1,) * (len(extent) - 1 - dim))
    return level


def normal_values(key, shape, scale, limit, cuts=(), held_as=jnp.bfloat16):
    values = scale * jax.random.normal(key, shape, jnp.float32)
    if cuts:
        values = values * block_levels(key, shape, cuts, -0.22, 0.18)
    return jnp.clip(values, -limit, limit).astype(held_as)


def noise_with(own_key, dims, scale, reach, shards, heavy, held_as=jnp.bfloat16):
    drawn = scale * jax.random.normal(own_key, dims, jnp.float32)
    if shards:
        drawn = drawn * block_levels(own_key, dims, shards, -0.22, 0.18)
    return jnp.clip(spiked(drawn, jax.random.fold_in(own_key, 3), *heavy), -reach, reach).astype(held_as)


def setup_inputs(seed: int = 0) -> dict:
    key_of = jax.random.split(jax.random.key(seed), 17)
    return {
        "tokens": noise_with(key_of[0], (TOKEN_COUNT, MODEL_WIDTH), 1.0, 6.0, ((0, 16),), (0, 1, 16, 2.0)),
        "cotangent": noise_with(key_of[1], (TOKEN_COUNT, MODEL_WIDTH), 1.0, 6.0, ((0, 16),), (0, 1, 16, 2.0)),
        "sequence_begin": draw_sequence_begin(jax.random.fold_in(key_of[16], 71), 0),
        "piece": draw_piece(jax.random.fold_in(key_of[16], 71), 0),
        "padding_length": draw_padding_length(jax.random.fold_in(key_of[16], 71), 0),
        "attn_gain": jnp.clip(0.5 + 1.0 * jax.random.uniform(key_of[5], (MODEL_WIDTH,), jnp.float32) ** block_levels(key_of[5], (MODEL_WIDTH,), ((0, 16),), -0.2, 0.2), 0.5, 1.5).astype(jnp.bfloat16),
        "q_gain": jnp.clip(0.5 + 1.5 * jax.random.uniform(key_of[6], (HEAD_SIZE,), jnp.float32) ** block_levels(key_of[6], (HEAD_SIZE,), ((0, 16),), -0.2, 0.2), 0.5, 2.0).astype(jnp.bfloat16),
        "k_gain": jnp.clip(0.5 + 1.5 * jax.random.uniform(key_of[7], (HEAD_SIZE,), jnp.float32) ** block_levels(key_of[7], (HEAD_SIZE,), ((0, 16),), -0.2, 0.2), 0.5, 2.0).astype(jnp.bfloat16),
        "w_query": normal_values(key_of[8], (MODEL_WIDTH, QUERY_HEADS * HEAD_SIZE), MODEL_WIDTH ** -0.5, 0.125, ((0, 16), (1, 2))),
        "key_weight": normal_values(key_of[9], (MODEL_WIDTH, VALUE_HEADS * HEAD_SIZE), MODEL_WIDTH ** -0.5, 0.125, ((0, 16), (1, 2))),
        "value_weight": normal_values(key_of[10], (MODEL_WIDTH, VALUE_HEADS * HEAD_SIZE), MODEL_WIDTH ** -0.5, 0.125, ((0, 16), (1, 2))),
        "w_out": normal_values(key_of[11], (MODEL_WIDTH, QUERY_HEADS * HEAD_SIZE), (QUERY_HEADS * HEAD_SIZE // 64) ** -0.5, 1.0, ((0, 16), (1, 2))),
        "mlp_gain": jnp.clip(0.5 + 1.0 * jax.random.uniform(key_of[12], (MODEL_WIDTH,), jnp.float32) ** block_levels(key_of[12], (MODEL_WIDTH,), ((0, 16),), -0.2, 0.2), 0.5, 1.5).astype(jnp.bfloat16),
        "w_gate": normal_values(key_of[13], (MODEL_WIDTH, FF), MODEL_WIDTH ** -0.5, 0.125, ((0, 16), (1, 2))),
        "w_up": normal_values(key_of[14], (MODEL_WIDTH, FF), MODEL_WIDTH ** -0.5, 0.125, ((0, 16), (1, 2))),
        "w_down": normal_values(key_of[15], (MODEL_WIDTH, FF), FF ** -0.5, 0.078125, ((0, 16), (1, 2))),
    }


EPS = 1e-06
THETA = 1000000.0
MASK_FILL = -1e+30
HIGH = lax.Precision.HIGHEST

@jax.custom_vjp
def lowered_forward(v):
    return lax.optimization_barrier(v.astype(jnp.bfloat16)).astype(jnp.float32)

@jax.custom_vjp
def lowered_backward(v):
    return v

def low_keep(v):
    return (lowered_forward(v), None)

def low_pass(kept, grad):
    return (grad,)

def back_keep(v):
    return (v, None)

def back_low(kept, grad):
    return (lowered_forward(grad),)
lowered_forward.defvjp(low_keep, low_pass)
lowered_backward.defvjp(back_keep, back_low)

def rms_scale(features, gain_vec):
    inverse = lax.rsqrt(lax.optimization_barrier(jnp.mean(features * features, axis=-1, keepdims=True)) + EPS)
    return features * inverse * gain_vec

def rotate(features, cosine, sine):
    half_width = features.shape[-1] // 2
    turned = jnp.concatenate([-features[..., half_width:], features[..., :half_width]], axis=-1)
    return features * cosine + turned * sine

def rope_tables(positions, width):
    half_width = width // 2
    frequency = THETA ** (-(jnp.arange(half_width, dtype=jnp.float32) * 2.0 / width))
    angles = positions[:, None] * frequency[None, :]
    angles = jnp.concatenate([angles, angles], axis=-1)
    return (jnp.cos(angles)[:, None, :], jnp.sin(angles)[:, None, :])

def allowed(query_index, key_index, start_query, start_key, piece_query, piece_key, key_live):
    same_doc = start_query[:, None] == start_key[None, :]
    causal_pair = key_index[None, :] <= query_index[:, None]
    picture_pair = (piece_query[:, None] == piece_key[None, :]) & (piece_query[:, None] > 0)
    live_key = key_live[None, :] | (key_index[None, :] == query_index[:, None])
    return same_doc & (causal_pair | picture_pair) & live_key

def matrix_product(left_side, right_side):
    return jnp.dot(left_side, right_side, precision=HIGH)

def matmul_t(left_side, right_side):
    return lax.dot_general(left_side, right_side, (((1,), (1,)), ((), ())), precision=HIGH)

def group_attention(pack_tokens):
    q_group, k_group, v_group, seq_group, piece_group, pad_count = pack_tokens
    group_rows = q_group.shape[0]
    key_index = jnp.arange(group_rows, dtype=jnp.int32)
    key_live = key_index < group_rows - pad_count
    pairs = allowed(key_index, key_index, seq_group, seq_group, piece_group, piece_group, key_live)
    kv_heads = k_group.shape[1]
    q_split = q_group.reshape(group_rows, kv_heads, -1, HEAD_SIZE)
    raw_scores = jnp.einsum('qkrd,skd->qkrs', q_split, k_group, precision=HIGH) * HEAD_SIZE ** (-0.5)
    scores = jnp.where(pairs[:, None, None, :], lowered_backward(raw_scores), MASK_FILL)
    prob_rows = lowered_forward(jax.nn.softmax(scores, axis=-1))
    head_out = jnp.einsum('qkrs,skd->qkrd', prob_rows, v_group, precision=HIGH)
    return lowered_backward(lowered_forward(head_out)).reshape(group_rows, -1, HEAD_SIZE)

def reference(tokens, cotangent, sequence_begin, piece, padding_length, attn_gain, q_gain, k_gain, w_query, key_weight, value_weight, w_out, mlp_gain, w_gate, w_up, w_down):
    position = jnp.arange(TOKEN_COUNT, dtype=jnp.int32) % GROUP_TOKENS
    cosine, sine = rope_tables((position - sequence_begin).astype(jnp.float32), HEAD_SIZE)

    def forward(x_rows, g_attn, g_query, g_key, wq_full, key_weight_whole, value_weight_whole, wo_full, g_mlp, wg_full, wu_full, wd_full):
        normed_input = lowered_forward(rms_scale(x_rows, g_attn))
        q_raw = lowered_backward(matrix_product(normed_input, wq_full)).reshape(TOKEN_COUNT, QUERY_HEADS, HEAD_SIZE)
        key_unrotated = lowered_backward(matrix_product(normed_input, key_weight_whole)).reshape(TOKEN_COUNT, VALUE_HEADS, HEAD_SIZE)
        query_ready = lowered_backward(lowered_forward(rotate(rms_scale(q_raw, g_query), cosine, sine)))
        key_ready = lowered_backward(lowered_forward(rotate(rms_scale(key_unrotated, g_key), cosine, sine)))
        value_ready = lowered_backward(lowered_forward(matrix_product(normed_input, value_weight_whole))).reshape(TOKEN_COUNT, VALUE_HEADS, HEAD_SIZE)
        pack_tokens = (query_ready.reshape(N_FSDP, GROUP_TOKENS, QUERY_HEADS, HEAD_SIZE), key_ready.reshape(N_FSDP, GROUP_TOKENS, VALUE_HEADS, HEAD_SIZE), value_ready.reshape(N_FSDP, GROUP_TOKENS, VALUE_HEADS, HEAD_SIZE), sequence_begin.reshape(N_FSDP, GROUP_TOKENS), piece.reshape(N_FSDP, GROUP_TOKENS), padding_length)
        head_out = lax.map(jax.checkpoint(group_attention), pack_tokens).reshape(TOKEN_COUNT, QUERY_HEADS * HEAD_SIZE)
        residual = x_rows + lowered_backward(matmul_t(head_out, wo_full))
        normed_two = lowered_forward(rms_scale(residual, g_mlp))
        gate_value = lowered_backward(matrix_product(normed_two, wg_full))
        up_value = lowered_backward(matrix_product(normed_two, wu_full))
        hidden = lowered_forward(jax.nn.silu(gate_value) * up_value)
        return residual + lowered_backward(matmul_t(hidden, wd_full))
    f32 = jnp.float32
    layer_out, pull = jax.vjp(forward, tokens.astype(f32), attn_gain.astype(f32), q_gain.astype(f32), k_gain.astype(f32), w_query.astype(f32), key_weight.astype(f32), value_weight.astype(f32), w_out.astype(f32), mlp_gain.astype(f32), w_gate.astype(f32), w_up.astype(f32), w_down.astype(f32))
    grads = pull(cotangent.astype(f32))
    return (layer_out.astype(jnp.bfloat16), grads[0].astype(jnp.bfloat16), grads[1], grads[2], grads[3], grads[4], grads[5], grads[6], grads[7], grads[8], grads[9], grads[10], grads[11])
```

```python
import functools

import jax
import jax.numpy as jnp
from jax import lax
from jax.experimental import pallas as pl
from jax.experimental.pallas import tpu as pltpu
from jax.experimental.layout import Layout, with_layout_constraint
from jax.sharding import PartitionSpec as P


HEAD_SIZE = 128


EPS = 1e-06
THETA = 1000000.0
MASK_FILL = -1e30
BOTH = ("fsdp", "ctx")
SIDE = 128
TAIL = 16
PIECE = 256
ROW_MAJOR = Layout(major_to_minor=(0, 1))


def rms_scale(features, gain_vec):
    inverse = lax.rsqrt(jnp.mean(features * features, axis=-1, keepdims=True) + EPS)
    return features * inverse * gain_vec


def rotate(features, cosine, sine):
    half_width = features.shape[-1] // 2
    turned = jnp.concatenate([-features[..., half_width:], features[..., :half_width]], axis=-1)
    return features * cosine + turned * sine


def rope_tables(positions, width):
    half_width = width // 2
    frequency = THETA ** (-(jnp.arange(half_width, dtype=jnp.float32) * 2.0 / width))
    angles = positions[:, None] * frequency[None, :]
    angles = jnp.concatenate([angles, angles], axis=-1)
    return (jnp.cos(angles)[:, None, :], jnp.sin(angles)[:, None, :])


def contract_last(left_side, right_side):
    return lax.dot_general(
        left_side, right_side, (((1,), (1,)), ((), ())), preferred_element_type=jnp.float32
    )


def contract_first(left_side, right_side):
    return lax.dot_general(
        left_side, right_side, (((0,), (0,)), ((), ())), preferred_element_type=jnp.float32
    )


def pair_sum(part, after=None):
    mine = part.astype(jnp.bfloat16)
    count = lax.axis_size("tp")
    total = mine.astype(jnp.float32)
    for step in range(1, count):
        ring = [(i, (i + step) % count) for i in range(count)]
        other = lax.ppermute(mine, "tp", ring)
        if after is not None:
            other, _ = lax.optimization_barrier((other, after))
        total = total + other.astype(jnp.float32)
    return total


def ring_order():
    outer, inner = lax.axis_size("fsdp"), lax.axis_size("ctx")
    cores = 2 if outer % 2 == 0 else 1
    lines = outer // cores
    chips = [(line, 0) for line in range(lines)]
    for turn, line in enumerate(reversed(range(lines))):
        across = range(1, inner) if turn % 2 == 0 else range(inner - 1, 0, -1)
        chips += [(line, place) for place in across]
    return [(line * cores + core) * inner + place for line, place in chips for core in range(cores)]


def take_blocks(features, order):
    size = features.shape[1] // len(order)
    return jnp.concatenate([features[:, i * size : (i + 1) * size] for i in order], axis=1)


def scatter_sum(part):
    return lax.psum_scatter(
        part, BOTH, scatter_dimension=0, tiled=True, axis_index_groups=[ring_order()]
    )


def gather_rows(shard):
    return lax.all_gather(shard, BOTH, axis=0, tiled=True, axis_index_groups=[ring_order()])


def swap_ctx(planes):
    return lax.all_to_all(planes, "ctx", split_axis=0, concat_axis=0, tiled=True)


def rope_kernel(q_heads, kv_heads, raw, cosine, sine, q_gain, k_gain, planes):
    count = planes.shape[0]
    for plane in range(count):
        sources = [plane * q_heads + h for h in range(q_heads)]
        sources += [count * q_heads + plane * kv_heads + h for h in range(kv_heads)]
        for i, source in enumerate(sources):
            gain = q_gain if i < q_heads else k_gain
            rows = raw[:, source * HEAD_SIZE : (source + 1) * HEAD_SIZE]
            scaled = rms_scale(rows, gain[...])
            turned = pltpu.roll(scaled, HEAD_SIZE // 2, 1)
            result = scaled * cosine[...] + turned * sine[...]
            planes[plane, :, i * HEAD_SIZE : (i + 1) * HEAD_SIZE] = result.astype(jnp.bfloat16)
        first = (count * (q_heads + kv_heads) + plane * kv_heads) * HEAD_SIZE
        wide = kv_heads * HEAD_SIZE
        values = raw[:, first : first + wide].astype(jnp.bfloat16)
        planes[plane, :, len(sources) * HEAD_SIZE :] = values


def to_heads(flat):
    count = lax.axis_size("ctx")
    return join_planes(flat.reshape(flat.shape[0], count, -1).transpose(1, 0, 2))


def join_planes(planes):
    moved = swap_ctx(planes)
    return moved.reshape(-1, moved.shape[2])


def to_tokens(joined, widths):
    count = lax.axis_size("ctx")
    moved = swap_ctx(joined.reshape(count, -1, joined.shape[1]))
    ends = [sum(widths[: i + 1]) for i in range(len(widths))]
    return [
        moved[:, :, end - wide : end].transpose(1, 0, 2).reshape(moved.shape[1], -1)
        for end, wide in zip(ends, widths)
    ]


def block_mask(low, start_col, start_row, piece_col, piece_row):
    rows = pl.ds(low, PIECE)
    own_start = start_col[rows, :]
    same = own_start == start_row[:, :low] if low else None
    left = lax.broadcasted_iota(jnp.int32, (PIECE, PIECE), 0)
    right = lax.broadcasted_iota(jnp.int32, (PIECE, PIECE), 1)
    own_piece = piece_col[rows, :]
    near = (right <= left) | ((own_piece == piece_row[:, low : low + PIECE]) & (own_piece > 0))
    near = near & ((own_start == start_row[:, low : low + PIECE]) | (left == right))
    return near if same is None else jnp.concatenate([same, near], axis=1)


def head_cols(ref, rows, heads):
    return jnp.concatenate(
        [ref[rows, h * HEAD_SIZE : (h + 1) * HEAD_SIZE] for h in heads], axis=0
    )


def masked_scores(q_rows, k_rows, mask, group):
    scores = contract_last(q_rows, k_rows) * HEAD_SIZE ** (-0.5)
    return jnp.where(jnp.concatenate([mask] * group, axis=0), scores, MASK_FILL)


def forward_kernel(q_heads, kv_heads, qkv, start_col, start_row, piece_col, piece_row, out, lse):
    group = q_heads // kv_heads
    for low in range(0, qkv.shape[0], PIECE):
        rows, high = pl.ds(low, PIECE), low + PIECE
        mask = block_mask(low, start_col, start_row, piece_col, piece_row)
        for c in range(kv_heads):
            heads = range(c * group, (c + 1) * group)
            k_rows = head_cols(qkv, pl.ds(0, high), [q_heads + c])
            v_rows = head_cols(qkv, pl.ds(0, high), [q_heads + kv_heads + c])
            scores = masked_scores(head_cols(qkv, rows, heads), k_rows, mask, group)
            row_max = jnp.max(scores, axis=-1, keepdims=True)
            expo = jnp.exp(scores - row_max)
            total = jnp.sum(expo, axis=-1, keepdims=True)
            probs = (expo * (1.0 / total)).astype(jnp.bfloat16)
            result = jnp.dot(probs, v_rows, preferred_element_type=jnp.float32)
            log_total = row_max + jnp.log(total)
            for i, h in enumerate(heads):
                part = slice(i * PIECE, (i + 1) * PIECE)
                out[rows, h * HEAD_SIZE : (h + 1) * HEAD_SIZE] = result[part].astype(jnp.bfloat16)
                lse[rows, h : h + 1] = log_total[part]


def backward_kernel(
    q_heads, kv_heads, qkv, d_out, lse, start_col, start_row, piece_col, piece_row, grads, k_sum, v_sum
):
    group = q_heads // kv_heads
    scale = HEAD_SIZE ** (-0.5)
    k_sum[...] = jnp.zeros_like(k_sum)
    v_sum[...] = jnp.zeros_like(v_sum)
    for low in range(0, qkv.shape[0], PIECE):
        rows, high = pl.ds(low, PIECE), low + PIECE
        mask = block_mask(low, start_col, start_row, piece_col, piece_row)
        for c in range(kv_heads):
            heads = range(c * group, (c + 1) * group)
            keys = pl.ds(0, high)
            k_rows = head_cols(qkv, keys, [q_heads + c])
            v_rows = head_cols(qkv, keys, [q_heads + kv_heads + c])
            q_rows = head_cols(qkv, rows, heads)
            d_rows = head_cols(d_out, rows, heads)
            totals = jnp.concatenate([lse[rows, h : h + 1] for h in heads], axis=0)
            probs = jnp.exp(masked_scores(q_rows, k_rows, mask, group) - totals)
            d_probs = contract_last(d_rows, v_rows)
            delta = jnp.sum(probs * d_probs, axis=-1, keepdims=True)
            d_scores = (probs * (d_probs - delta)).astype(jnp.bfloat16)
            d_query = jnp.dot(d_scores, k_rows, preferred_element_type=jnp.float32) * scale
            for i, h in enumerate(heads):
                part = d_query[i * PIECE : (i + 1) * PIECE]
                grads[rows, h * HEAD_SIZE : (h + 1) * HEAD_SIZE] = part.astype(jnp.bfloat16)
            cols = slice(c * HEAD_SIZE, (c + 1) * HEAD_SIZE)
            k_sum[keys, cols] += contract_first(d_scores, q_rows)
            v_sum[keys, cols] += contract_first(probs.astype(jnp.bfloat16), d_rows)
    middle = (q_heads + kv_heads) * HEAD_SIZE
    grads[:, q_heads * HEAD_SIZE : middle] = (k_sum[...] * scale).astype(jnp.bfloat16)
    grads[:, middle:] = v_sum[...].astype(jnp.bfloat16)


def attention_call(kernel, results, scratch, work, args):
    rows, heads = args[0].shape[0], work
    pairs = rows * (rows + PIECE) // 2 * heads
    return pl.pallas_call(
        kernel,
        out_shape=results,
        in_specs=[pl.BlockSpec(memory_space=pltpu.VMEM)] * len(args),
        out_specs=[pl.BlockSpec(memory_space=pltpu.VMEM)] * len(results),
        scratch_shapes=scratch,
        cost_estimate=pl.CostEstimate(
            flops=pairs * HEAD_SIZE * 16,
            transcendentals=pairs,
            bytes_accessed=sum(a.size * a.dtype.itemsize for a in args),
        ),
        compiler_params=pltpu.CompilerParams(vmem_limit_bytes=56 * 1024 * 1024),
    )(*args)


def body(
    tokens,
    cotangent,
    sequence_begin,
    piece,
    padding_length,
    attn_gain,
    q_gain,
    k_gain,
    w_query,
    key_weight,
    value_weight,
    w_out,
    mlp_gain,
    w_gate,
    w_up,
    w_down,
):
    f32 = jnp.float32
    bf16 = jnp.bfloat16
    tok_rows = tokens.shape[0]
    group_rows = sequence_begin.shape[0]
    offset = lax.axis_index("ctx") * tok_rows
    local_index = offset + jnp.arange(tok_rows, dtype=jnp.int32)
    my_start = lax.dynamic_slice_in_dim(sequence_begin, offset, tok_rows)
    cosine, sine = rope_tables((local_index - my_start).astype(f32), HEAD_SIZE)
    key_index = jnp.arange(group_rows, dtype=jnp.int32)
    key_live = key_index < group_rows - padding_length[0]

    def head_prep(raw_heads, gain_vec):
        return rotate(rms_scale(raw_heads, gain_vec), cosine, sine)

    order = ring_order()
    back = [order.index(i) for i in range(len(order))]
    place = (jnp.array(order)[:, None] == jnp.arange(len(order))[None, :]).astype(f32)
    tokens = take_blocks(tokens, order)
    cotangent = take_blocks(cotangent, order)
    width = tokens.shape[1]
    tp_cols = w_query.shape[1]
    kv_cols = key_weight.shape[1]
    qkv_cols = tp_cols + 2 * kv_cols
    rows = attn_gain.shape[0]
    ff_cols = w_gate.shape[1]
    small = q_gain.shape[0]
    side_index = lax.broadcasted_iota(jnp.int32, (rows, SIDE), 1)
    side = jnp.zeros((rows, SIDE), bf16)
    short = ((0, rows - small),)
    gains = (attn_gain, mlp_gain, jnp.pad(q_gain, short), jnp.pad(k_gain, short))
    for i, gain in enumerate(gains):
        side = jnp.where(side_index == i, gain[:, None], side)
    shards = width // rows
    w_qkv = jnp.concatenate([w_query, key_weight, value_weight, side], axis=1)
    qkv_full = gather_rows(w_qkv)
    wo_full = gather_rows(w_out)
    gu_full = gather_rows(jnp.concatenate([w_gate, w_up], axis=1))
    wd_full = gather_rows(w_down)
    side_full = qkv_full[:, qkv_cols:]
    g_attn, g_mlp = side_full[:, 0], side_full[:, 1]
    head_side = side_full.reshape(shards, rows, SIDE)[:, :small, 2:4]
    head_side = jnp.sum(place[:, :, None, None] * head_side[:, None].astype(f32), axis=0)
    g_query = head_side[..., 0].reshape(-1)
    g_key = head_side[..., 1].reshape(-1)
    attn_gain_f = g_attn.astype(f32)
    qgain_f = g_query.astype(f32)
    kgain_f = g_key.astype(f32)
    x_rows = tokens.astype(f32)
    normed_bf = rms_scale(x_rows, attn_gain_f).astype(bf16)
    qkv_raw = jnp.dot(normed_bf, qkv_full, preferred_element_type=f32)
    q_raw = qkv_raw[:, :tp_cols].reshape(tok_rows, -1, HEAD_SIZE)
    key_unrotated = qkv_raw[:, tp_cols : tp_cols + kv_cols].reshape(tok_rows, -1, HEAD_SIZE)
    ctx_count = lax.axis_size("ctx")
    q_wide, kv_wide = tp_cols // ctx_count, kv_cols // ctx_count
    q_heads, kv_heads = q_wide // HEAD_SIZE, kv_wide // HEAD_SIZE
    lower = jnp.arange(HEAD_SIZE) < HEAD_SIZE // 2
    planes = pl.pallas_call(
        functools.partial(rope_kernel, q_heads, kv_heads),
        name="rope",
        out_shape=jax.ShapeDtypeStruct((ctx_count, tok_rows, q_wide + 2 * kv_wide), bf16),
        in_specs=[pl.BlockSpec(memory_space=pltpu.VMEM)] * 5,
        out_specs=pl.BlockSpec(memory_space=pltpu.VMEM),
        cost_estimate=pl.CostEstimate(
            flops=16 * qkv_raw.size, transcendentals=0, bytes_accessed=6 * qkv_raw.size
        ),
    )(
        qkv_raw,
        cosine[:, 0],
        jnp.where(lower, -sine[:, 0], sine[:, 0]),
        qgain_f[None],
        kgain_f[None],
    )
    joined = join_planes(planes)
    masks = (
        sequence_begin[:, None],
        jnp.where(key_live, sequence_begin, -1)[None, :],
        piece[:, None],
        piece[None, :],
    )
    o_head, log_totals = attention_call(
        functools.partial(forward_kernel, q_heads, kv_heads),
        [
            jax.ShapeDtypeStruct((group_rows, q_wide), bf16),
            jax.ShapeDtypeStruct((group_rows, q_heads), f32),
        ],
        [],
        q_heads,
        (joined, *masks),
    )
    (o_tok,) = to_tokens(o_head, [q_wide])
    residual = x_rows + pair_sum(contract_last(o_tok, wo_full))
    mlp_gain_f = g_mlp.astype(f32)
    normed_two = rms_scale(residual, mlp_gain_f).astype(bf16)
    gate_up = jnp.dot(normed_two, gu_full, preferred_element_type=f32)
    gate_value = gate_up[:, :ff_cols]
    up_value = gate_up[:, ff_cols:]
    gate_sigmoid = jax.nn.sigmoid(gate_value)
    gate_silu = gate_value * gate_sigmoid
    hidden = (gate_silu * up_value).astype(bf16)
    down_part = contract_last(hidden, wd_full).astype(bf16)
    grad_down_part = with_layout_constraint(
        contract_first(cotangent, hidden).astype(bf16), ROW_MAJOR
    )
    grad_down_part, cotangent = lax.optimization_barrier((grad_down_part, cotangent))
    grad_down = scatter_sum(grad_down_part)
    d_hidden = jnp.dot(cotangent, wd_full, preferred_element_type=f32)
    d_gate = (
        d_hidden * up_value * gate_sigmoid * (1.0 + gate_value * (1.0 - gate_sigmoid))
    ).astype(bf16)
    d_up = (d_hidden * gate_silu).astype(bf16)
    d_gate_up = jnp.concatenate([d_gate, d_up], axis=1)
    grad_gate_up_part = contract_first(normed_two, d_gate_up).astype(bf16)
    d_norm_two = pair_sum(contract_last(d_gate_up, gu_full))
    grad_gate_up_part, down_part, d_norm_two = lax.optimization_barrier(
        (grad_gate_up_part, down_part, d_norm_two)
    )
    grad_gate_up = scatter_sum(grad_gate_up_part)
    layer_out = residual + pair_sum(down_part)
    layer_out = take_blocks(layer_out.astype(bf16), back)
    _, pull_two = jax.vjp(rms_scale, residual, mlp_gain_f)
    d_residual, d_mlp_gain = pull_two(d_norm_two)
    d_residual = d_residual + cotangent.astype(f32)
    d_branch = d_residual.astype(bf16)
    grad_out_part = contract_first(d_branch, o_tok).astype(bf16)
    grad_out_part, d_branch = lax.optimization_barrier((grad_out_part, d_branch))
    grad_out = scatter_sum(grad_out_part)
    d_out = (
        jnp.dot(d_branch, wo_full, preferred_element_type=f32)
        .astype(bf16)
    )
    d_head = to_heads(d_out)

    (d_joined,) = attention_call(
        functools.partial(backward_kernel, q_heads, kv_heads),
        [jax.ShapeDtypeStruct(joined.shape, bf16)],
        [pltpu.VMEM((group_rows, kv_wide), f32)] * 2,
        q_heads,
        (joined, d_head, log_totals, *masks),
    )
    dq_tok, dk_tok, dv_flat = to_tokens(d_joined, [q_wide, kv_wide, kv_wide])
    dq_tok = dq_tok.reshape(tok_rows, -1, HEAD_SIZE)
    dk_tok = dk_tok.reshape(tok_rows, -1, HEAD_SIZE)
    _, pull_query = jax.vjp(head_prep, q_raw, qgain_f)
    dq_raw, d_qgain = pull_query(dq_tok.astype(f32))
    _, pull_key = jax.vjp(head_prep, key_unrotated, kgain_f)
    dk_raw, d_kgain = pull_key(dk_tok.astype(f32))
    dq_flat = dq_raw.astype(bf16).reshape(tok_rows, -1)
    dk_flat = dk_raw.astype(bf16).reshape(tok_rows, -1)
    picks = (jnp.arange(TAIL)[:, None] == jnp.arange(SIDE)[None, :]).astype(bf16)
    d_qkv = jnp.concatenate(
        [
            jnp.concatenate([part, jnp.zeros((TAIL, part.shape[1]), bf16)], axis=0)
            for part in (dq_flat, dk_flat, dv_flat)
        ]
        + [jnp.concatenate([jnp.zeros((tok_rows, SIDE), bf16), picks], axis=0)],
        axis=1,
    )
    d_norm_part = contract_last(d_qkv, qkv_full)[:tok_rows].astype(bf16)
    _, pull_one = jax.vjp(rms_scale, x_rows, attn_gain_f)
    _, d_attn_gain = pull_one(d_norm_part.astype(f32))
    d_norm = pair_sum(d_norm_part, d_attn_gain)
    d_tokens, _ = pull_one(d_norm)
    grad_tokens = take_blocks((d_residual + d_tokens).astype(bf16), back)
    head_grads = jnp.stack([d_qgain, d_kgain]).reshape(2, 1, shards, small)
    head_grads = jnp.sum(place[None, :, :, None] * head_grads, axis=2)
    head_grads = jnp.pad(head_grads, ((0, 0), (0, 0), (0, rows - small)))
    gain_rows = jnp.concatenate(
        [d_attn_gain[None], d_mlp_gain[None] / lax.axis_size("tp"), head_grads.reshape(2, width)]
    )
    gain_rows = jnp.pad(gain_rows, ((0, TAIL - 4), (0, 0)))
    gain_rows = pair_sum(gain_rows)
    normed_tail = jnp.concatenate([normed_bf, gain_rows.astype(bf16)], axis=0)
    grad_qkv_part = contract_first(normed_tail, d_qkv).astype(bf16)
    grad_qkv_part = with_layout_constraint(grad_qkv_part, ROW_MAJOR)
    grad_qkv = scatter_sum(grad_qkv_part)
    grad_side = grad_qkv[:, qkv_cols:]
    side_sums = grad_side[:, :4].astype(f32)
    return (
        layer_out,
        grad_tokens,
        side_sums[:, 0],
        side_sums[:small, 2],
        side_sums[:small, 3],
        grad_qkv[:, :tp_cols].astype(f32),
        grad_qkv[:, tp_cols : tp_cols + kv_cols].astype(f32),
        grad_qkv[:, tp_cols + kv_cols : qkv_cols].astype(f32),
        grad_out.astype(f32),
        grad_side[:, 1].astype(f32),
        grad_gate_up[:, :ff_cols].astype(f32),
        grad_gate_up[:, ff_cols:].astype(f32),
        grad_down.astype(f32),
    )


def solution(mesh):
    in_specs = (
        P(("fsdp", "ctx"), None),
        P(("fsdp", "ctx"), None),
        P("fsdp"),
        P("fsdp"),
        P("fsdp"),
        P(("fsdp", "ctx")),
        P(("fsdp", "ctx")),
        P(("fsdp", "ctx")),
        P(("fsdp", "ctx"), "tp"),
        P(("fsdp", "ctx"), "tp"),
        P(("fsdp", "ctx"), "tp"),
        P(("fsdp", "ctx"), "tp"),
        P(("fsdp", "ctx")),
        P(("fsdp", "ctx"), "tp"),
        P(("fsdp", "ctx"), "tp"),
        P(("fsdp", "ctx"), "tp"),
    )
    out_specs = (
        P(("fsdp", "ctx"), None),
        P(("fsdp", "ctx"), None),
        P(("fsdp", "ctx")),
        P(("fsdp", "ctx")),
        P(("fsdp", "ctx")),
        P(("fsdp", "ctx"), "tp"),
        P(("fsdp", "ctx"), "tp"),
        P(("fsdp", "ctx"), "tp"),
        P(("fsdp", "ctx"), "tp"),
        P(("fsdp", "ctx")),
        P(("fsdp", "ctx"), "tp"),
        P(("fsdp", "ctx"), "tp"),
        P(("fsdp", "ctx"), "tp"),
    )

    return jax.shard_map(body, mesh=mesh, in_specs=in_specs, out_specs=out_specs, check_vma=False)
```

```python
import functools

import jax
import jax.numpy as jnp
from jax import lax
from jax.experimental import pallas as pl
from jax.experimental.pallas import tpu as pltpu
from jax.experimental.layout import Layout, with_layout_constraint
from jax.sharding import PartitionSpec as P


HEAD_SIZE = 128


EPS = 1e-06
THETA = 1000000.0
MASK_FILL = -1e30
BOTH = ("fsdp", "ctx")
SIDE = 128
TAIL = 16
PIECE = 256
ROW_MAJOR = Layout(major_to_minor=(0, 1))


def rms_scale(features, gain_vec):
    inverse = lax.rsqrt(jnp.mean(features * features, axis=-1, keepdims=True) + EPS)
    return features * inverse * gain_vec


def rotate(features, cosine, sine):
    half_width = features.shape[-1] // 2
    turned = jnp.concatenate([-features[..., half_width:], features[..., :half_width]], axis=-1)
    return features * cosine + turned * sine


def rope_tables(positions, width):
    half_width = width // 2
    frequency = THETA ** (-(jnp.arange(half_width, dtype=jnp.float32) * 2.0 / width))
    angles = positions[:, None] * frequency[None, :]
    angles = jnp.concatenate([angles, angles], axis=-1)
    return (jnp.cos(angles)[:, None, :], jnp.sin(angles)[:, None, :])


def contract_last(left_side, right_side):
    return lax.dot_general(
        left_side, right_side, (((1,), (1,)), ((), ())), preferred_element_type=jnp.float32
    )


def contract_first(left_side, right_side):
    return lax.dot_general(
        left_side, right_side, (((0,), (0,)), ((), ())), preferred_element_type=jnp.float32
    )


def pair_sum(part, after=None):
    mine = part.astype(jnp.bfloat16)
    count = lax.axis_size("tp")
    total = mine.astype(jnp.float32)
    for step in range(1, count):
        ring = [(i, (i + step) % count) for i in range(count)]
        other = lax.ppermute(mine, "tp", ring)
        if after is not None:
            other, _ = lax.optimization_barrier((other, after))
        total = total + other.astype(jnp.float32)
    return total


def ring_order():
    outer, inner = lax.axis_size("fsdp"), lax.axis_size("ctx")
    cores = 2 if outer % 2 == 0 else 1
    lines = outer // cores
    chips = [(line, 0) for line in range(lines)]
    for turn, line in enumerate(reversed(range(lines))):
        across = range(1, inner) if turn % 2 == 0 else range(inner - 1, 0, -1)
        chips += [(line, place) for place in across]
    return [(line * cores + core) * inner + place for line, place in chips for core in range(cores)]


def take_blocks(features, order):
    size = features.shape[1] // len(order)
    return jnp.concatenate([features[:, i * size : (i + 1) * size] for i in order], axis=1)


def scatter_sum(part):
    return lax.psum_scatter(
        part, BOTH, scatter_dimension=0, tiled=True, axis_index_groups=[ring_order()]
    )


def gather_rows(shard):
    return lax.all_gather(shard, BOTH, axis=0, tiled=True, axis_index_groups=[ring_order()])


def swap_ctx(planes):
    return lax.all_to_all(planes, "ctx", split_axis=0, concat_axis=0, tiled=True)


def rope_kernel(q_heads, kv_heads, raw, cosine, sine, q_gain, k_gain, planes):
    count = planes.shape[0]
    for plane in range(count):
        sources = [plane * q_heads + h for h in range(q_heads)]
        sources += [count * q_heads + plane * kv_heads + h for h in range(kv_heads)]
        for i, source in enumerate(sources):
            gain = q_gain if i < q_heads else k_gain
            rows = raw[:, source * HEAD_SIZE : (source + 1) * HEAD_SIZE]
            scaled = rms_scale(rows, gain[...])
            turned = pltpu.roll(scaled, HEAD_SIZE // 2, 1)
            result = scaled * cosine[...] + turned * sine[...]
            planes[plane, :, i * HEAD_SIZE : (i + 1) * HEAD_SIZE] = result.astype(jnp.bfloat16)
        first = (count * (q_heads + kv_heads) + plane * kv_heads) * HEAD_SIZE
        wide = kv_heads * HEAD_SIZE
        values = raw[:, first : first + wide].astype(jnp.bfloat16)
        planes[plane, :, len(sources) * HEAD_SIZE :] = values


def to_heads(flat):
    count = lax.axis_size("ctx")
    return join_planes(flat.reshape(flat.shape[0], count, -1).transpose(1, 0, 2))


def join_planes(planes):
    moved = swap_ctx(planes)
    return moved.reshape(-1, moved.shape[2])


def to_tokens(joined, widths):
    count = lax.axis_size("ctx")
    moved = swap_ctx(joined.reshape(count, -1, joined.shape[1]))
    ends = [sum(widths[: i + 1]) for i in range(len(widths))]
    return [
        moved[:, :, end - wide : end].transpose(1, 0, 2).reshape(moved.shape[1], -1)
        for end, wide in zip(ends, widths)
    ]


def block_mask(low, start_col, start_row, piece_col, piece_row):
    rows = pl.ds(low, PIECE)
    own_start = start_col[rows, :]
    same = own_start == start_row[:, :low] if low else None
    left = lax.broadcasted_iota(jnp.int32, (PIECE, PIECE), 0)
    right = lax.broadcasted_iota(jnp.int32, (PIECE, PIECE), 1)
    own_piece = piece_col[rows, :]
    near = (right <= left) | ((own_piece == piece_row[:, low : low + PIECE]) & (own_piece > 0))
    near = near & ((own_start == start_row[:, low : low + PIECE]) | (left == right))
    return near if same is None else jnp.concatenate([same, near], axis=1)


def head_cols(ref, rows, heads):
    return jnp.concatenate(
        [ref[rows, h * HEAD_SIZE : (h + 1) * HEAD_SIZE] for h in heads], axis=0
    )


def masked_scores(q_rows, k_rows, mask, group):
    scores = contract_last(q_rows, k_rows) * HEAD_SIZE ** (-0.5)
    return jnp.where(jnp.concatenate([mask] * group, axis=0), scores, MASK_FILL)


def forward_kernel(q_heads, kv_heads, qkv, start_col, start_row, piece_col, piece_row, out, lse):
    group = q_heads // kv_heads
    for low in range(0, qkv.shape[0], PIECE):
        rows, high = pl.ds(low, PIECE), low + PIECE
        mask = block_mask(low, start_col, start_row, piece_col, piece_row)
        for c in range(kv_heads):
            heads = range(c * group, (c + 1) * group)
            k_rows = head_cols(qkv, pl.ds(0, high), [q_heads + c])
            v_rows = head_cols(qkv, pl.ds(0, high), [q_heads + kv_heads + c])
            scores = masked_scores(head_cols(qkv, rows, heads), k_rows, mask, group)
            row_max = jnp.max(scores, axis=-1, keepdims=True)
            expo = jnp.exp(scores - row_max)
            total = jnp.sum(expo, axis=-1, keepdims=True)
            probs = (expo * (1.0 / total)).astype(jnp.bfloat16)
            result = jnp.dot(probs, v_rows, preferred_element_type=jnp.float32)
            log_total = row_max + jnp.log(total)
            for i, h in enumerate(heads):
                part = slice(i * PIECE, (i + 1) * PIECE)
                out[rows, h * HEAD_SIZE : (h + 1) * HEAD_SIZE] = result[part].astype(jnp.bfloat16)
                lse[rows, h : h + 1] = log_total[part]


def backward_kernel(
    q_heads, kv_heads, qkv, d_out, lse, start_col, start_row, piece_col, piece_row, grads, k_sum, v_sum
):
    group = q_heads // kv_heads
    scale = HEAD_SIZE ** (-0.5)
    k_sum[...] = jnp.zeros_like(k_sum)
    v_sum[...] = jnp.zeros_like(v_sum)
    for low in range(0, qkv.shape[0], PIECE):
        rows, high = pl.ds(low, PIECE), low + PIECE
        mask = block_mask(low, start_col, start_row, piece_col, piece_row)
        for c in range(kv_heads):
            heads = range(c * group, (c + 1) * group)
            keys = pl.ds(0, high)
            k_rows = head_cols(qkv, keys, [q_heads + c])
            v_rows = head_cols(qkv, keys, [q_heads + kv_heads + c])
            q_rows = head_cols(qkv, rows, heads)
            d_rows = head_cols(d_out, rows, heads)
            totals = jnp.concatenate([lse[rows, h : h + 1] for h in heads], axis=0)
            probs = jnp.exp(masked_scores(q_rows, k_rows, mask, group) - totals)
            d_probs = contract_last(d_rows, v_rows)
            delta = jnp.sum(probs * d_probs, axis=-1, keepdims=True)
            d_scores = (probs * (d_probs - delta)).astype(jnp.bfloat16)
            d_query = jnp.dot(d_scores, k_rows, preferred_element_type=jnp.float32) * scale
            for i, h in enumerate(heads):
                part = d_query[i * PIECE : (i + 1) * PIECE]
                grads[rows, h * HEAD_SIZE : (h + 1) * HEAD_SIZE] = part.astype(jnp.bfloat16)
            cols = slice(c * HEAD_SIZE, (c + 1) * HEAD_SIZE)
            k_sum[keys, cols] += contract_first(d_scores, q_rows)
            v_sum[keys, cols] += contract_first(probs.astype(jnp.bfloat16), d_rows)
    middle = (q_heads + kv_heads) * HEAD_SIZE
    grads[:, q_heads * HEAD_SIZE : middle] = (k_sum[...] * scale).astype(jnp.bfloat16)
    grads[:, middle:] = v_sum[...].astype(jnp.bfloat16)


def attention_call(kernel, results, scratch, work, args):
    rows, heads = args[0].shape[0], work
    pairs = rows * (rows + PIECE) // 2 * heads
    return pl.pallas_call(
        kernel,
        out_shape=results,
        in_specs=[pl.BlockSpec(memory_space=pltpu.VMEM)] * len(args),
        out_specs=[pl.BlockSpec(memory_space=pltpu.VMEM)] * len(results),
        scratch_shapes=scratch,
        cost_estimate=pl.CostEstimate(
            flops=pairs * HEAD_SIZE * 16,
            transcendentals=pairs,
            bytes_accessed=sum(a.size * a.dtype.itemsize for a in args),
        ),
        compiler_params=pltpu.CompilerParams(vmem_limit_bytes=56 * 1024 * 1024),
    )(*args)


def body(
    tokens,
    cotangent,
    sequence_begin,
    piece,
    padding_length,
    attn_gain,
    q_gain,
    k_gain,
    w_query,
    key_weight,
    value_weight,
    w_out,
    mlp_gain,
    w_gate,
    w_up,
    w_down,
):
    f32 = jnp.float32
    bf16 = jnp.bfloat16
    tok_rows = tokens.shape[0]
    group_rows = sequence_begin.shape[0]
    offset = lax.axis_index("ctx") * tok_rows
    local_index = offset + jnp.arange(tok_rows, dtype=jnp.int32)
    my_start = lax.dynamic_slice_in_dim(sequence_begin, offset, tok_rows)
    cosine, sine = rope_tables((local_index - my_start).astype(f32), HEAD_SIZE)
    key_index = jnp.arange(group_rows, dtype=jnp.int32)
    key_live = key_index < group_rows - padding_length[0]

    def head_prep(raw_heads, gain_vec):
        return rotate(rms_scale(raw_heads, gain_vec), cosine, sine)

    order = ring_order()
    back = [order.index(i) for i in range(len(order))]
    place = (jnp.array(order)[:, None] == jnp.arange(len(order))[None, :]).astype(f32)
    tokens = take_blocks(tokens, order)
    cotangent = take_blocks(cotangent, order)
    width = tokens.shape[1]
    tp_cols = w_query.shape[1]
    kv_cols = key_weight.shape[1]
    qkv_cols = tp_cols + 2 * kv_cols
    rows = attn_gain.shape[0]
    ff_cols = w_gate.shape[1]
    small = q_gain.shape[0]
    side_index = lax.broadcasted_iota(jnp.int32, (rows, SIDE), 1)
    side = jnp.zeros((rows, SIDE), bf16)
    short = ((0, rows - small),)
    gains = (attn_gain, mlp_gain, jnp.pad(q_gain, short), jnp.pad(k_gain, short))
    for i, gain in enumerate(gains):
        side = jnp.where(side_index == i, gain[:, None], side)
    shards = width // rows
    w_qkvo = jnp.concatenate([w_query, key_weight, value_weight, side, w_out], axis=1)
    qkvo_full = gather_rows(w_qkvo)
    qkv_full = qkvo_full[:, : qkv_cols + SIDE]
    wo_full = qkvo_full[:, qkv_cols + SIDE :]
    gu_full = gather_rows(jnp.concatenate([w_gate, w_up], axis=1))
    wd_full = gather_rows(w_down)
    side_full = qkv_full[:, qkv_cols:]
    g_attn, g_mlp = side_full[:, 0], side_full[:, 1]
    head_side = side_full.reshape(shards, rows, SIDE)[:, :small, 2:4]
    head_side = jnp.sum(place[:, :, None, None] * head_side[:, None].astype(f32), axis=0)
    g_query = head_side[..., 0].reshape(-1)
    g_key = head_side[..., 1].reshape(-1)
    attn_gain_f = g_attn.astype(f32)
    qgain_f = g_query.astype(f32)
    kgain_f = g_key.astype(f32)
    x_rows = tokens.astype(f32)
    normed_bf = rms_scale(x_rows, attn_gain_f).astype(bf16)
    qkv_raw = jnp.dot(normed_bf, qkv_full, preferred_element_type=f32)
    q_raw = qkv_raw[:, :tp_cols].reshape(tok_rows, -1, HEAD_SIZE)
    key_unrotated = qkv_raw[:, tp_cols : tp_cols + kv_cols].reshape(tok_rows, -1, HEAD_SIZE)
    ctx_count = lax.axis_size("ctx")
    q_wide, kv_wide = tp_cols // ctx_count, kv_cols // ctx_count
    q_heads, kv_heads = q_wide // HEAD_SIZE, kv_wide // HEAD_SIZE
    lower = jnp.arange(HEAD_SIZE) < HEAD_SIZE // 2
    planes = pl.pallas_call(
        functools.partial(rope_kernel, q_heads, kv_heads),
        name="rope",
        out_shape=jax.ShapeDtypeStruct((ctx_count, tok_rows, q_wide + 2 * kv_wide), bf16),
        in_specs=[pl.BlockSpec(memory_space=pltpu.VMEM)] * 5,
        out_specs=pl.BlockSpec(memory_space=pltpu.VMEM),
        cost_estimate=pl.CostEstimate(
            flops=16 * qkv_raw.size, transcendentals=0, bytes_accessed=6 * qkv_raw.size
        ),
    )(
        qkv_raw,
        cosine[:, 0],
        jnp.where(lower, -sine[:, 0], sine[:, 0]),
        qgain_f[None],
        kgain_f[None],
    )
    joined = join_planes(planes)
    masks = (
        sequence_begin[:, None],
        jnp.where(key_live, sequence_begin, -1)[None, :],
        piece[:, None],
        piece[None, :],
    )
    o_head, log_totals = attention_call(
        functools.partial(forward_kernel, q_heads, kv_heads),
        [
            jax.ShapeDtypeStruct((group_rows, q_wide), bf16),
            jax.ShapeDtypeStruct((group_rows, q_heads), f32),
        ],
        [],
        q_heads,
        (joined, *masks),
    )
    (o_tok,) = to_tokens(o_head, [q_wide])
    residual = x_rows + pair_sum(contract_last(o_tok, wo_full))
    mlp_gain_f = g_mlp.astype(f32)
    normed_two = rms_scale(residual, mlp_gain_f).astype(bf16)
    gate_up = jnp.dot(normed_two, gu_full, preferred_element_type=f32)
    gate_value = gate_up[:, :ff_cols]
    up_value = gate_up[:, ff_cols:]
    gate_sigmoid = jax.nn.sigmoid(gate_value)
    gate_silu = gate_value * gate_sigmoid
    hidden = (gate_silu * up_value).astype(bf16)
    down_part = contract_last(hidden, wd_full).astype(bf16)
    grad_down_part = with_layout_constraint(
        contract_first(cotangent, hidden).astype(bf16), ROW_MAJOR
    )
    grad_down_part, cotangent = lax.optimization_barrier((grad_down_part, cotangent))
    grad_down = scatter_sum(grad_down_part)
    d_hidden = jnp.dot(cotangent, wd_full, preferred_element_type=f32)
    d_gate = (
        d_hidden * up_value * gate_sigmoid * (1.0 + gate_value * (1.0 - gate_sigmoid))
    ).astype(bf16)
    d_up = (d_hidden * gate_silu).astype(bf16)
    d_gate_up = jnp.concatenate([d_gate, d_up], axis=1)
    grad_gate_up_part = contract_first(normed_two, d_gate_up).astype(bf16)
    d_norm_two = pair_sum(contract_last(d_gate_up, gu_full))
    grad_gate_up_part, down_part, d_norm_two = lax.optimization_barrier(
        (grad_gate_up_part, down_part, d_norm_two)
    )
    grad_gate_up = scatter_sum(grad_gate_up_part)
    layer_out = residual + pair_sum(down_part)
    layer_out = take_blocks(layer_out.astype(bf16), back)
    _, pull_two = jax.vjp(rms_scale, residual, mlp_gain_f)
    d_residual, d_mlp_gain = pull_two(d_norm_two)
    d_residual = d_residual + cotangent.astype(f32)
    d_branch = d_residual.astype(bf16)
    grad_out_part = contract_first(d_branch, o_tok).astype(bf16)
    grad_out_part, d_branch = lax.optimization_barrier((grad_out_part, d_branch))
    d_out = (
        jnp.dot(d_branch, wo_full, preferred_element_type=f32)
        .astype(bf16)
    )
    d_head = to_heads(d_out)

    (d_joined,) = attention_call(
        functools.partial(backward_kernel, q_heads, kv_heads),
        [jax.ShapeDtypeStruct(joined.shape, bf16)],
        [pltpu.VMEM((group_rows, kv_wide), f32)] * 2,
        q_heads,
        (joined, d_head, log_totals, *masks),
    )
    dq_tok, dk_tok, dv_flat = to_tokens(d_joined, [q_wide, kv_wide, kv_wide])
    dq_tok = dq_tok.reshape(tok_rows, -1, HEAD_SIZE)
    dk_tok = dk_tok.reshape(tok_rows, -1, HEAD_SIZE)
    _, pull_query = jax.vjp(head_prep, q_raw, qgain_f)
    dq_raw, d_qgain = pull_query(dq_tok.astype(f32))
    _, pull_key = jax.vjp(head_prep, key_unrotated, kgain_f)
    dk_raw, d_kgain = pull_key(dk_tok.astype(f32))
    dq_flat = dq_raw.astype(bf16).reshape(tok_rows, -1)
    dk_flat = dk_raw.astype(bf16).reshape(tok_rows, -1)
    picks = (jnp.arange(TAIL)[:, None] == jnp.arange(SIDE)[None, :]).astype(bf16)
    d_qkv = jnp.concatenate(
        [
            jnp.concatenate([part, jnp.zeros((TAIL, part.shape[1]), bf16)], axis=0)
            for part in (dq_flat, dk_flat, dv_flat)
        ]
        + [jnp.concatenate([jnp.zeros((tok_rows, SIDE), bf16), picks], axis=0)],
        axis=1,
    )
    d_norm_part = contract_last(d_qkv, qkv_full)[:tok_rows].astype(bf16)
    _, pull_one = jax.vjp(rms_scale, x_rows, attn_gain_f)
    _, d_attn_gain = pull_one(d_norm_part.astype(f32))
    d_norm = pair_sum(d_norm_part, d_attn_gain)
    d_tokens, _ = pull_one(d_norm)
    grad_tokens = take_blocks((d_residual + d_tokens).astype(bf16), back)
    head_grads = jnp.stack([d_qgain, d_kgain]).reshape(2, 1, shards, small)
    head_grads = jnp.sum(place[None, :, :, None] * head_grads, axis=2)
    head_grads = jnp.pad(head_grads, ((0, 0), (0, 0), (0, rows - small)))
    gain_rows = jnp.concatenate(
        [d_attn_gain[None], d_mlp_gain[None] / lax.axis_size("tp"), head_grads.reshape(2, width)]
    )
    gain_rows = jnp.pad(gain_rows, ((0, TAIL - 4), (0, 0)))
    gain_rows = pair_sum(gain_rows)
    normed_tail = jnp.concatenate([normed_bf, gain_rows.astype(bf16)], axis=0)
    grad_qkv_part = contract_first(normed_tail, d_qkv).astype(bf16)
    grad_qkv_part = jnp.concatenate([grad_qkv_part, grad_out_part], axis=1)
    grad_qkv_part = with_layout_constraint(grad_qkv_part, ROW_MAJOR)
    grad_qkv = scatter_sum(grad_qkv_part)
    grad_out = grad_qkv[:, qkv_cols + SIDE :]
    grad_side = grad_qkv[:, qkv_cols : qkv_cols + SIDE]
    side_sums = grad_side[:, :4].astype(f32)
    return (
        layer_out,
        grad_tokens,
        side_sums[:, 0],
        side_sums[:small, 2],
        side_sums[:small, 3],
        grad_qkv[:, :tp_cols].astype(f32),
        grad_qkv[:, tp_cols : tp_cols + kv_cols].astype(f32),
        grad_qkv[:, tp_cols + kv_cols : qkv_cols].astype(f32),
        grad_out.astype(f32),
        grad_side[:, 1].astype(f32),
        grad_gate_up[:, :ff_cols].astype(f32),
        grad_gate_up[:, ff_cols:].astype(f32),
        grad_down.astype(f32),
    )


def solution(mesh):
    in_specs = (
        P(("fsdp", "ctx"), None),
        P(("fsdp", "ctx"), None),
        P("fsdp"),
        P("fsdp"),
        P("fsdp"),
        P(("fsdp", "ctx")),
        P(("fsdp", "ctx")),
        P(("fsdp", "ctx")),
        P(("fsdp", "ctx"), "tp"),
        P(("fsdp", "ctx"), "tp"),
        P(("fsdp", "ctx"), "tp"),
        P(("fsdp", "ctx"), "tp"),
        P(("fsdp", "ctx")),
        P(("fsdp", "ctx"), "tp"),
        P(("fsdp", "ctx"), "tp"),
        P(("fsdp", "ctx"), "tp"),
    )
    out_specs = (
        P(("fsdp", "ctx"), None),
        P(("fsdp", "ctx"), None),
        P(("fsdp", "ctx")),
        P(("fsdp", "ctx")),
        P(("fsdp", "ctx")),
        P(("fsdp", "ctx"), "tp"),
        P(("fsdp", "ctx"), "tp"),
        P(("fsdp", "ctx"), "tp"),
        P(("fsdp", "ctx"), "tp"),
        P(("fsdp", "ctx")),
        P(("fsdp", "ctx"), "tp"),
        P(("fsdp", "ctx"), "tp"),
        P(("fsdp", "ctx"), "tp"),
    )

    return jax.shard_map(body, mesh=mesh, in_specs=in_specs, out_specs=out_specs, check_vma=False)
```
